32 devices in a mesh: phase: 4 (over y, x), line: 8 (over z, core).
Axes of the slice: x: 2, y: 2, z: 4, core: 2. Of those that a mesh axis runs over, the one named last changes fastest.
Arguments:
- signal: bfloat16 [4, 8, 8192, 256], P('phase', 'line'), may hold values from -8 to 8, as said below
- tap_gain: float32 [3, 256], replicated, may hold values from 0.3 to 1.2
Outputs:
- echoed: bfloat16 [4, 8, 8192, 256], P('phase', 'line')
The draws below stay inside these ranges and needn't reach their ends.
Inputs may be any that keep to these rules, and one draw needn't show every extreme that they name: signal holds numbers from -8 to 8.
All inputs are finite; a program needn't handle non-finite values.
Results may differ from the reference program's by a relative error of at most 0.0055.
Values may be sent and summed in bfloat16 or wider, within the bound.
A program may use at most 64 MiB of HBM per device.

```python
import jax
import jax.numpy as jnp
from jax import lax

STEPS_DEV = 8192
CHANNELS = 256
SEGMENTS = 4
RECORDS = 8


def draw_signal(key, part):
    keys = jax.random.split(key, 2)
    loud = jnp.exp(jax.random.uniform(keys[0], (SEGMENTS, RECORDS, 1, CHANNELS), jnp.float32, -1.2, 1.2))
    noise = jax.random.normal(keys[1], (SEGMENTS, RECORDS, STEPS_DEV, CHANNELS), jnp.float32)
    return jnp.clip(loud * noise, -8.0, 8.0).astype(jnp.bfloat16)


def setup_inputs(seed: int = 0) -> dict:
    arg_keys = jax.random.split(jax.random.key(seed), 3)
    signal = draw_signal(jax.random.fold_in(arg_keys[2], 71), 0)
    tap_gain = jnp.clip(jax.random.uniform(arg_keys[1], (3, CHANNELS), jnp.float32, 0.3, 1.2), 0.3, 1.2)
    return {"signal": signal, "tap_gain": tap_gain}


def reference(signal, tap_gain):
    wide_in = signal.astype(jnp.float32)
    mixed = tap_gain[0] * wide_in + tap_gain[1] * jnp.roll(wide_in, 2, axis=0) + tap_gain[2] * jnp.roll(wide_in, 3, axis=0)
    power = lax.optimization_barrier(jnp.mean(mixed * mixed, axis=(0, 2), keepdims=True))
    echoed = (mixed * lax.rsqrt(power + 1e-05)).astype(jnp.bfloat16)
    return echoed
```

```python
import functools

import jax
import jax.numpy as jnp
from jax import lax
from jax.experimental import pallas as pl
from jax.experimental.pallas import tpu as pltpu
from jax.sharding import PartitionSpec as P

MESH = pl.DeviceIdType.MESH
CHUNK_ROWS = 256
LAG = 2
SUB_ROWS = 64
STORE_ROWS = 512


def exchange_kernel(
    n, chunk, signal_ref, gain_ref, mixed_ref, scale_ref,
    near, far, sums, load_sem, out1_sem, in1_sem, out2_sem, in2_sem, sum_out, sum_in,
):
    me = lax.axis_index("phase")
    rows = near.shape[1]
    steps = rows // chunk
    to_1 = lax.rem(me + 2, n)
    if n == 4:
        odd = lax.rem(me, 2)
        to_2 = me + 1 - 2 * odd
        held = 1 - odd
    else:
        to_2 = lax.rem(me + 3, n)
        held = 0

    def part(k):
        return pl.ds(pl.multiple_of(k * chunk, chunk), chunk)

    def load(k):
        return pltpu.make_async_copy(
            signal_ref.at[0, 0, part(k)], near.at[0, part(k)], load_sem.at[k]
        )

    def send_1(k):
        return pltpu.make_async_remote_copy(
            src_ref=near.at[0, part(k)], dst_ref=near.at[1, part(k)],
            send_sem=out1_sem.at[k], recv_sem=in1_sem.at[k],
            device_id={"phase": to_1}, device_id_type=MESH,
        )

    def send_2(k):
        return pltpu.make_async_remote_copy(
            src_ref=near.at[held, part(k)], dst_ref=far.at[part(k)],
            send_sem=out2_sem.at[k], recv_sem=in2_sem.at[k],
            device_id={"phase": to_2}, device_id_type=MESH,
        )

    def send_sum(d):
        return pltpu.make_async_remote_copy(
            src_ref=sums.at[0], dst_ref=sums.at[d],
            send_sem=sum_out.at[d], recv_sem=sum_in.at[d],
            device_id={"phase": lax.rem(me + d, n)}, device_id_type=MESH,
        )

    def each(body):
        lax.fori_loop(0, steps, lambda k, c: (body(k), c)[1], 0)

    each(lambda k: load(k).start())
    barrier = pltpu.get_barrier_semaphore()
    for d in range(1, n):
        pl.semaphore_signal(
            barrier, inc=1, device_id={"phase": lax.rem(me + d, n)}, device_id_type=MESH
        )
    pl.semaphore_wait(barrier, n - 1)

    def first(k):
        load(k).wait()
        send_1(k).start()

    each(first)

    g0, g1, g2 = (gain_ref[pl.ds(i, 1), :] for i in range(3))

    def mix(k, total):
        send_2(k).wait_recv()
        for j in range(chunk // SUB_ROWS):
            at = pl.ds(pl.multiple_of(k * chunk + j * SUB_ROWS, SUB_ROWS), SUB_ROWS)
            mixed = (
                g0 * near[0, at, :].astype(jnp.float32)
                + g1 * near[1, at, :].astype(jnp.float32)
                + g2 * far[at, :].astype(jnp.float32)
            )
            mixed_ref[at, :] = mixed
            total = total + jnp.sum((mixed * mixed).reshape(SUB_ROWS // 8, 8, -1), axis=0)
        return total

    def pass_on(k):
        send_1(k).wait_recv()
        send_2(k).start()

    def step(k, total):
        pass_on(k)
        return mix(k - LAG, total)

    lax.fori_loop(0, LAG, lambda k, c: (pass_on(k), c)[1], 0)
    total = lax.fori_loop(LAG, steps, step, jnp.zeros(sums.shape[1:], jnp.float32))
    total = lax.fori_loop(steps - LAG, steps, mix, total)

    sums[0] = total
    for d in range(1, n):
        send_sum(d).start()
    for d in range(1, n):
        send_sum(d).wait_recv()
    for d in range(1, n):
        total = total + sums[d]
    power = jnp.sum(total, axis=0, keepdims=True) * (1.0 / (rows * n))
    scale_ref[...] = lax.rsqrt(power + 1e-5)

    def last(k):
        send_1(k).wait_send()
        send_2(k).wait_send()

    each(last)
    for d in range(1, n):
        send_sum(d).wait_send()


def scale_kernel(mixed_ref, scale_ref, out_ref):
    size = out_ref.shape[2]
    start = pl.multiple_of(pl.program_id(0) * size, size)
    out_ref[0, 0] = (mixed_ref[pl.ds(start, size), :] * scale_ref[...]).astype(out_ref.dtype)


def per_device(n, signal, tap_gain):
    _, _, rows, channels = signal.shape
    chunk = CHUNK_ROWS
    while rows % chunk:
        chunk //= 2
    steps = rows // chunk
    vmem = pl.BlockSpec(memory_space=pltpu.VMEM)
    dma = pltpu.SemaphoreType.DMA
    mixed, scale = pl.pallas_call(
        functools.partial(exchange_kernel, n, chunk),
        out_shape=(
            pltpu.VMEM((rows, channels), jnp.float32),
            pltpu.VMEM((1, channels), jnp.float32),
        ),
        in_specs=[pl.BlockSpec(memory_space=pltpu.HBM), vmem],
        out_specs=(vmem, vmem),
        scratch_shapes=[
            pltpu.VMEM((2, rows, channels), signal.dtype),
            pltpu.VMEM((rows, channels), signal.dtype),
            pltpu.VMEM((n, 8, channels), jnp.float32),
            dma((steps,)), dma((steps,)), dma((steps,)), dma((steps,)), dma((steps,)),
            dma((n,)), dma((n,)),
        ],
        compiler_params=pltpu.CompilerParams(
            collective_id=0, has_side_effects=True, vmem_limit_bytes=32 * 2**20
        ),
        name="exchange",
    )(signal, tap_gain)
    size = min(STORE_ROWS, rows)
    return pl.pallas_call(
        scale_kernel,
        grid=(rows // size,),
        out_shape=jax.ShapeDtypeStruct(signal.shape, jnp.bfloat16),
        in_specs=[vmem, vmem],
        out_specs=pl.BlockSpec((1, 1, size, channels), lambda i: (0, 0, i, 0)),
        compiler_params=pltpu.CompilerParams(vmem_limit_bytes=16 * 2**20),
        name="rescale",
    )(mixed, scale)


def solution(mesh):
    return jax.shard_map(
        functools.partial(per_device, mesh.shape["phase"]),
        mesh=mesh,
        in_specs=(P("phase", "line", None, None), P()),
        out_specs=P("phase", "line", None, None),
        check_vma=False,
    )
```

```python
import functools

import jax
import jax.numpy as jnp
from jax import lax
from jax.experimental import pallas as pl
from jax.experimental.pallas import tpu as pltpu
from jax.sharding import PartitionSpec as P

MESH = pl.DeviceIdType.MESH
CHUNK_ROWS = 256
LAG = 2
SUB_ROWS = 64
STORE_ROWS = 1024


def exchange_kernel(
    n, chunk, signal_ref, gain_ref, mixed_ref, scale_ref,
    near, far, sums, load_sem, out1_sem, in1_sem, out2_sem, in2_sem, sum_out, sum_in,
):
    me = lax.axis_index("phase")
    rows = near.shape[1]
    steps = rows // chunk
    to_1 = lax.rem(me + 2, n)
    if n == 4:
        odd = lax.rem(me, 2)
        to_2 = me + 1 - 2 * odd
        held = 1 - odd
    else:
        to_2 = lax.rem(me + 3, n)
        held = 0

    def part(k):
        return pl.ds(pl.multiple_of(k * chunk, chunk), chunk)

    def load(k):
        return pltpu.make_async_copy(
            signal_ref.at[0, 0, part(k)], near.at[0, part(k)], load_sem.at[k]
        )

    def send_1(k):
        return pltpu.make_async_remote_copy(
            src_ref=near.at[0, part(k)], dst_ref=near.at[1, part(k)],
            send_sem=out1_sem.at[k], recv_sem=in1_sem.at[k],
            device_id={"phase": to_1}, device_id_type=MESH,
        )

    def send_2(k):
        return pltpu.make_async_remote_copy(
            src_ref=near.at[held, part(k)], dst_ref=far.at[part(k)],
            send_sem=out2_sem.at[k], recv_sem=in2_sem.at[k],
            device_id={"phase": to_2}, device_id_type=MESH,
        )

    def send_sum(d):
        return pltpu.make_async_remote_copy(
            src_ref=sums.at[0], dst_ref=sums.at[d],
            send_sem=sum_out.at[d], recv_sem=sum_in.at[d],
            device_id={"phase": lax.rem(me + d, n)}, device_id_type=MESH,
        )

    def each(body):
        lax.fori_loop(0, steps, lambda k, c: (body(k), c)[1], 0)

    each(lambda k: load(k).start())
    barrier = pltpu.get_barrier_semaphore()
    for d in range(1, n):
        pl.semaphore_signal(
            barrier, inc=1, device_id={"phase": lax.rem(me + d, n)}, device_id_type=MESH
        )
    pl.semaphore_wait(barrier, n - 1)

    def first(k):
        load(k).wait()
        send_1(k).start()

    each(first)

    g0, g1, g2 = (gain_ref[pl.ds(i, 1), :] for i in range(3))

    def mix(k, total):
        send_2(k).wait_recv()
        for j in range(chunk // SUB_ROWS):
            at = pl.ds(pl.multiple_of(k * chunk + j * SUB_ROWS, SUB_ROWS), SUB_ROWS)
            mixed = (
                g0 * near[0, at, :].astype(jnp.float32)
                + g1 * near[1, at, :].astype(jnp.float32)
                + g2 * far[at, :].astype(jnp.float32)
            )
            mixed_ref[at, :] = mixed
            total = total + jnp.sum((mixed * mixed).reshape(SUB_ROWS // 8, 8, -1), axis=0)
        return total

    def pass_on(k):
        send_1(k).wait_recv()
        send_2(k).start()

    def step(k, total):
        pass_on(k)
        return mix(k - LAG, total)

    lax.fori_loop(0, LAG, lambda k, c: (pass_on(k), c)[1], 0)
    total = lax.fori_loop(LAG, steps, step, jnp.zeros(sums.shape[1:], jnp.float32))
    total = lax.fori_loop(steps - LAG, steps, mix, total)

    sums[0] = total
    for d in range(1, n):
        send_sum(d).start()
    for d in range(1, n):
        send_sum(d).wait_recv()
    for d in range(1, n):
        total = total + sums[d]
    power = jnp.sum(total, axis=0, keepdims=True) * (1.0 / (rows * n))
    scale_ref[...] = lax.rsqrt(power + 1e-5)

    def last(k):
        send_1(k).wait_send()
        send_2(k).wait_send()

    each(last)
    for d in range(1, n):
        send_sum(d).wait_send()


def scale_kernel(size, mixed_ref, scale_ref, out_ref, held, sem):
    def store(k):
        at = pl.ds(pl.multiple_of(k * size, size), size)
        return pltpu.make_async_copy(held.at[at], out_ref.at[0, 0, at], sem.at[k])

    scale = scale_ref[...]

    def step(k, c):
        for j in range(size // SUB_ROWS):
            at = pl.ds(pl.multiple_of(k * size + j * SUB_ROWS, SUB_ROWS), SUB_ROWS)
            held[at, :] = (mixed_ref[at, :] * scale).astype(held.dtype)
        store(k).start()
        return c

    def finish(k, c):
        store(k).wait()
        return c

    blocks = held.shape[0] // size
    lax.fori_loop(0, blocks, step, 0)
    lax.fori_loop(0, blocks, finish, 0)


def per_device(n, signal, tap_gain):
    _, _, rows, channels = signal.shape
    chunk = CHUNK_ROWS
    while rows % chunk:
        chunk //= 2
    steps = rows // chunk
    vmem = pl.BlockSpec(memory_space=pltpu.VMEM)
    dma = pltpu.SemaphoreType.DMA
    mixed, scale = pl.pallas_call(
        functools.partial(exchange_kernel, n, chunk),
        out_shape=(
            pltpu.VMEM((rows, channels), jnp.float32),
            pltpu.VMEM((1, channels), jnp.float32),
        ),
        in_specs=[pl.BlockSpec(memory_space=pltpu.HBM), vmem],
        out_specs=(vmem, vmem),
        scratch_shapes=[
            pltpu.VMEM((2, rows, channels), signal.dtype),
            pltpu.VMEM((rows, channels), signal.dtype),
            pltpu.VMEM((n, 8, channels), jnp.float32),
            dma((steps,)), dma((steps,)), dma((steps,)), dma((steps,)), dma((steps,)),
            dma((n,)), dma((n,)),
        ],
        compiler_params=pltpu.CompilerParams(
            collective_id=0, has_side_effects=True, vmem_limit_bytes=54 * 2**20
        ),
        name="exchange",
    )(signal, tap_gain)
    size = STORE_ROWS
    while rows % size:
        size //= 2
    return pl.pallas_call(
        functools.partial(scale_kernel, size),
        out_shape=jax.ShapeDtypeStruct(signal.shape, jnp.bfloat16),
        in_specs=[vmem, vmem],
        out_specs=pl.BlockSpec(memory_space=pltpu.HBM),
        scratch_shapes=[
            pltpu.VMEM((rows, channels), jnp.bfloat16),
            dma((rows // size,)),
        ],
        compiler_params=pltpu.CompilerParams(vmem_limit_bytes=16 * 2**20),
        name="rescale",
    )(mixed, scale)


def solution(mesh):
    return jax.shard_map(
        functools.partial(per_device, mesh.shape["phase"]),
        mesh=mesh,
        in_specs=(P("phase", "line", None, None), P()),
        out_specs=P("phase", "line", None, None),
        check_vma=False,
    )
```
